32 devices in a mesh: row: 8 (over y, x, core), col: 4 (over z).
Axes of the slice: x: 2, y: 2, z: 4, core: 2. Of those that a mesh axis runs over, the one named last changes fastest.
Arguments:
- surface: bfloat16 [16384, 16384], P('row', 'col'), may hold values from -0.0234375 to 0.0234375
- excitation: float32 [16384, 128], P(('row', 'col')), may hold values from -6 to 6
- dtn_blocks: bfloat16 [32, 1024, 1024], P(('row', 'col')), may hold values from -0.09375 to 0.09375
- interp_blocks: bfloat16 [32, 1024, 2048], P(('row', 'col')), may hold values from -0.09375 to 0.09375
- adjacency: int32 [32, 6], P(('row', 'col')), may hold values from 0 to 31, as said below
Outputs:
- solution: float32 [16384, 128], P(('row', 'col'))
- residual: float32 [16384, 128], P(('row', 'col'))
The draws below stay inside these ranges and needn't reach their ends.
Inputs may be any that keep to these rules, and one draw needn't show every extreme that they name: `adjacency`: entry [s, k] names a subdomain of the same spatial group as s (equal index // 4); it may name s itself, which adds nothing.
All inputs are finite; a program needn't handle non-finite values.
Results may differ from the reference program's by a relative error of at most 0.02.
Values may be sent and summed in bfloat16 or wider, within the bound.
A program may use at most 64 MiB of HBM per device.

```python
import jax
import jax.numpy as jnp
from jax import lax

NS = 16384
M = 1024
NE = 128
ITERS = 2
NADJ = 6
NSUB = 32
GROUP = 4
RB = 2048
N_ROW = 8


def draw_adjacency(key, part):
    base = jnp.arange(NSUB, dtype=jnp.int32) // GROUP * GROUP
    offsets = jax.random.randint(jax.random.fold_in(key, 17), (NSUB, NADJ), 0, GROUP, dtype=jnp.int32)
    return base[:, None] + offsets


def block_scale(stream_key, shape, cuts, smallest, top_value):
    factor_of = 1.0
    for axis_at, shards_of in cuts:
        steps = jax.random.uniform(jax.random.fold_in(jax.random.fold_in(stream_key, 6), axis_at), (shards_of,), jnp.float32, smallest / len(cuts), top_value / len(cuts))
        factor_of = factor_of * jnp.repeat(jnp.exp(steps), shape[axis_at] // shards_of).reshape((-1,) + (1,) * (len(shape) - 1 - axis_at))
    return factor_of


def gaussian(stream_key, shape, deviation, reach, shards=(), held_as=jnp.bfloat16):
    result = deviation * jax.random.normal(stream_key, shape, jnp.float32)
    if shards:
        result = result * block_scale(stream_key, shape, shards, -0.22, 0.18)
    return jnp.clip(result, -reach, reach).astype(held_as)


def setup_inputs(seed: int = 0) -> dict:
    seeds = jax.random.split(jax.random.key(seed), 6)
    return {
        "surface": gaussian(seeds[0], (NS, NS), (4 * NS) ** -0.5, 0.0234375, ((0, 8), (1, 4))),
        "excitation": gaussian(seeds[1], (NS, NE), 1.0, 6.0, ((0, 32),), jnp.float32),
        "dtn_blocks": gaussian(seeds[2], (NSUB, M, M), (4 * M) ** -0.5, 0.09375, ((0, 32),)),
        "interp_blocks": gaussian(seeds[3], (NSUB, M, RB), (2 * RB) ** -0.5, 0.09375, ((0, 32),)),
        "adjacency": draw_adjacency(jax.random.fold_in(seeds[5], 71), 0),
    }


damping = 0.25
face_weight = 0.25


def reference(surface, excitation, dtn_blocks, interp_blocks, adjacency):
    current = excitation
    residual = excitation
    indices = jnp.arange(NSUB, dtype=jnp.int32)
    for sweep in range(ITERS):
        rounded = current.astype(jnp.bfloat16)
        applied = jnp.dot(surface, rounded, preferred_element_type=jnp.float32)
        grouped = rounded.reshape(N_ROW, RB, NE)

        def trace_one(index):
            block = lax.dynamic_index_in_dim(grouped, index // GROUP, 0, keepdims=False)
            return jnp.dot(interp_blocks[index], block, preferred_element_type=jnp.float32).astype(jnp.bfloat16)

        traces = lax.map(trace_one, indices)

        def respond(index):
            own = traces[index]
            own_wide = own.astype(jnp.float32)
            neighbours = jnp.zeros((M, NE), jnp.float32)
            for slot in range(NADJ):
                neighbours = neighbours + traces[adjacency[index, slot]].astype(jnp.float32)
            combined = jnp.dot(dtn_blocks[index], own, preferred_element_type=jnp.float32) + own_wide
            combined = combined + face_weight * (NADJ * own_wide - neighbours)
            response = combined.astype(jnp.bfloat16)
            return lax.dot_general(interp_blocks[index], response, (((0,), (0,)), ((), ())), preferred_element_type=jnp.float32)

        returned = lax.map(respond, indices)
        back = returned.reshape(N_ROW, GROUP, RB, NE).sum(axis=1).reshape(NS, NE)
        residual = excitation - current - applied - back
        current = current + damping * residual
    return current, residual
```

```python
import functools

import jax
import jax.numpy as jnp
from jax import lax
from jax.experimental import pallas as pl
from jax.experimental.pallas import tpu as pltpu
from jax.sharding import PartitionSpec as P

ITERS = 2
NADJ = 6
STAGGER = 0

damping = 0.25
face_weight = 0.25
F32, BF16 = jnp.float32, jnp.bfloat16


def xor(a, b, bits):
    total = 0
    for i in range(bits):
        x, y = a // 2**i % 2, b // 2**i % 2
        total = total + (x + y - 2 * x * y) * 2**i
    return total


def gray(p, bits):
    return xor(p, p // 2, bits)


def ungray(g, bits):
    total, above = 0, 0
    for i in reversed(range(bits)):
        bit = g // 2**i % 2
        above = above + bit - 2 * above * bit
        total = total + above * 2**i
    return total


def kernel(
    R, n, pieces, tile,
    exc_hbm, interp_hbm, surf_hbm, dtn_hbm, adj,
    sol_ref, res_ref,
    exc, interp, surf, dtn, grp, colb, trc, acc, part, sbuf, rbuf, nbr, psend, precv, cnt,
    load_sem, g_ss, g_rs, t_ss, t_rs, c_ss, c_rs, h_ss, h_rs, r_ss, r_rs, p_ss, p_rs, n_ss, n_rs,
):
    bits = n.bit_length() - 1
    mid = n // 2
    _, _, hs, ne = grp.shape[1:]
    m, rb = interp.shape
    shard = 2 * hs
    ps = m // pieces
    r, c = lax.axis_index("row"), lax.axis_index("col")
    core, chip = r % 2, r // 2
    pos = ungray(xor(chip, c, bits), bits)
    right, left = (r, (c + 1) % n), (r, (c + n - 1) % n)
    partner = (chip * 2 + 1 - core, c)
    gnext = (xor(gray((pos + 1) % n, bits), c, bits) * 2 + core, c)
    gprev = (xor(gray((pos + n - 1) % n, bits), c, bits) * 2 + core, c)

    loads = [
        pltpu.make_async_copy(exc_hbm, exc, load_sem.at[0]),
        pltpu.make_async_copy(interp_hbm, interp, load_sem.at[1]),
    ]
    tiles = surf.shape[0] // tile
    for i in range(tiles):
        rows = pl.ds(i * tile, tile)
        loads.append(pltpu.make_async_copy(surf_hbm.at[rows], surf.at[rows], load_sem.at[3 + i]))
    loads.append(pltpu.make_async_copy(dtn_hbm, dtn, load_sem.at[2]))
    for load in loads:
        load.start()

    def counts_go(q, j):
        return (mid <= q < j) or (j < q <= mid - 1)

    barrier = pltpu.get_barrier_semaphore()

    def greet(device):
        pl.semaphore_signal(barrier, inc=1, device_id=device, device_id_type=pl.DeviceIdType.MESH)

    for device in (partner, gnext, gprev):
        greet(device)
    expected = 3
    for q in range(n):
        others = [j for j in range(n) if abs(q - j) == 1 or counts_go(q, j) or counts_go(j, q)]

        @pl.when(c == q)
        def _():
            for j in others:
                greet((r, j))

        expected = expected + jnp.where(c == q, len(others), 0)
    pl.semaphore_wait(barrier, expected)

    def remote(src, dst, ss, rs, device):
        return pltpu.make_async_remote_copy(
            src_ref=src, dst_ref=dst, send_sem=ss, recv_sem=rs,
            device_id=device, device_id_type=pl.DeviceIdType.MESH,
        )

    waits = []

    def later(condition, copy):
        waits.append((condition, copy))

    def hop(buf, ss, rs, s, d, t, p, receive=False):
        step = t if receive else t - 1
        owner = (c + n - step) % n if d == 0 else (c + step) % n
        block = buf.at[s, owner, p]
        return remote(block, block, ss.at[s, d, t - 1, p], rs.at[s, d, t - 1, p], right if d == 0 else left)

    def sends(d, t):
        if d == 0:
            return jnp.logical_and(c >= t - 1, c <= n - 2)
        return jnp.logical_and(c <= n - t, c >= 1)

    def receives(d, t):
        return c >= t if d == 0 else c <= n - 1 - t

    def valid(d, t):
        return (c >= 0) if t == 0 else receives(d, t)

    def owner_of(d, t):
        return (c + n - t) % n if d == 0 else (c + t) % n

    def chain_copies(src, s, owner, h):
        block = src.at[owner, h]
        dst = colb.at[s, core, owner, h]
        return (
            remote(block, dst, c_ss.at[s, owner, h], c_rs.at[s, owner, h], gnext if h == 0 else gprev),
            remote(block, dst, h_ss.at[s, owner, h], h_rs.at[s, owner, h], partner),
        )

    def slots(t):
        return [(0, 0)] if t == 0 else [(0, t), (1, t)]

    def chain_source(s, t):
        for d, t in slots(t):
            @pl.when(jnp.logical_and(pos == 0, valid(d, t)))
            def _():
                for h in range(2):
                    on, share = chain_copies(grp.at[s], s, owner_of(d, t), h)
                    on.start()
                    share.start()

    def chain_relay(s, tick):
        for q in range(1, n):
            todo = []
            for t in range(n):
                for h in range(2):
                    if t + (q if h == 0 else n - q) == tick:
                        todo += [(d, t, h) for d, t in slots(t)]
            for d, t, h in todo:
                @pl.when(jnp.logical_and(pos == q, valid(d, t)))
                def _():
                    on, share = chain_copies(colb.at[s, core], s, owner_of(d, t), h)
                    on.wait_recv()
                    if q != (n - 1 if h == 0 else 1):
                        on.start()
                    share.start()

    def chain_sent(s):
        for owner in range(n):
            for h in range(2):
                copies = functools.partial(chain_copies, colb.at[s, core], s, owner, h)
                later(lambda h=h: pos != (n - 1 if h == 0 else 1), lambda copies=copies: copies()[0])
                later(None, lambda copies=copies: copies()[1])

    def shared(s, owner):
        for h in range(2):
            block = colb.at[s, 1 - core, owner, h]
            remote(block, block, h_ss.at[s, owner, h], h_rs.at[s, owner, h], partner).wait_recv()

    ranks = [sorted(range(n), key=lambda o: (abs(o - q), o)) for q in range(n)]
    owner_at = []
    for k in range(n):
        owner = ranks[0][k]
        for q in range(1, n):
            owner = jnp.where(c == q, ranks[q][k], owner)
        owner_at.append(owner)

    for p in range(n):
        count = jnp.float32(0)
        for k in range(NADJ):
            count = count + jnp.where(adj[0, k] % n == p, 1.0, 0.0).astype(F32)
        cnt[c, p] = jnp.full((8, ne), count, F32)

    def count_copy(j, q):
        return remote(cnt.at[j], cnt.at[j], n_ss.at[q], n_rs.at[j], (r, q))

    for j in range(n):
        takers = [q for q in range(n) if counts_go(q, j)]
        if takers:
            @pl.when(c == j)
            def _():
                for q in takers:
                    count_copy(j, q).start()
            for q in takers:
                later(lambda j=j: c == j, lambda j=j, q=q: count_copy(j, q))

    def send_own(s, h, value):
        grp[s, c, h] = value.astype(BF16)
        for d in range(2):
            copy = hop(grp, g_ss, g_rs, s, d, 1, h)
            pl.when(sends(d, 1))(copy.start)
            later(lambda d=d: sends(d, 1), lambda d=d: hop(grp, g_ss, g_rs, s, d, 1, h))

    def gather(s):
        chain_source(s, 0)
        for t in range(1, n):
            for p in range(2):
                for d in range(2):
                    @pl.when(receives(d, t))
                    def _():
                        hop(grp, g_ss, g_rs, s, d, t, p, True).wait_recv()
                    if t < n - 1:
                        copy = hop(grp, g_ss, g_rs, s, d, t + 1, p)
                        pl.when(sends(d, t + 1))(copy.start)
                        later(
                            lambda d=d, t=t: sends(d, t + 1),
                            lambda d=d, t=t, p=p: hop(grp, g_ss, g_rs, s, d, t + 1, p),
                        )
            chain_source(s, t)
            chain_relay(s, t)

    def trace_sends(q, d, t):
        a = q if d == 0 else n - 1 - q
        return a <= mid - 1 and a >= t - 1

    def trace_receives(q, d, t):
        a = q if d == 0 else n - 1 - q
        return a <= mid and a >= t

    def trace_hop(s, q, d, t, p, receive=False):
        step = t if receive else t - 1
        owner = q - step if d == 0 else q + step
        block = trc.at[s, owner, p]
        to = (r, q + 1 if d == 0 else q - 1)
        return remote(block, block, t_ss.at[s, d, t - 1, p], t_rs.at[s, d, t - 1, p], to)

    def sum_copy(s, q, d, j, p):
        to = (r, q + 1 if d == 0 else q - 1)
        return remote(psend.at[s, d, j, p], precv.at[s, d, j, p], p_ss.at[s, d, j, p], p_rs.at[s, d, j, p], to)

    def send_traces(s, p):
        for q in range(n):
            @pl.when(c == q)
            def _():
                for d in range(2):
                    if trace_sends(q, d, 1) and 0 <= q + 1 - 2 * d < n:
                        trace_hop(s, q, d, 1, p).start()

    def weighted(s, j, p, owners):
        total = None
        for o in owners:
            term = cnt[j, o, 0:1] * trc[s, o, p].astype(F32)
            total = term if total is None else total + term
        return total

    def forward_traces(s, t):
        for q in range(n):
            todo = [d for d in range(2) if trace_sends(q, d, t + 1) and trace_receives(q, d, t)]
            if todo:
                @pl.when(c == q)
                def _():
                    for p in range(pieces):
                        for d in todo:
                            trace_hop(s, q, d, t, p, True).wait_recv()
                            trace_hop(s, q, d, t + 1, p).start()

    def trace_sums(s, ends):
        for q in range(n):
            far = [d for d in range(2) if (q if d == 0 else n - 1 - q) > mid]
            if bool(far) != ends:
                continue

            @pl.when(c == q)
            def _():
                if s == 0:
                    for j in range(n):
                        if counts_go(q, j):
                            count_copy(j, q).wait_recv()
                for p in range(pieces):
                    value = weighted(s, q, p, [q])
                    for d in range(2):
                        a = q if d == 0 else n - 1 - q
                        behind = list(range(q)) if d == 0 else list(range(q + 1, n))
                        ahead = list(range(n - 1, q, -1)) if d == 0 else list(range(q))
                        if a <= mid:
                            for t in range(1, a + 1):
                                if not (trace_sends(q, d, t + 1) and trace_receives(q, d, t)):
                                    trace_hop(s, q, d, t, p, True).wait_recv()
                        if a >= mid:
                            for j in ahead:
                                if a == mid:
                                    out = weighted(s, j, p, behind + [q])
                                else:
                                    sum_copy(s, q, d, j, p).wait_recv()
                                    out = precv[s, d, j, p].astype(F32) + weighted(s, j, p, [q])
                                psend[s, d, j, p] = out.astype(BF16)
                                sum_copy(s, q, d, j, p).start()
                                later(lambda q=q: c == q, functools.partial(sum_copy, s, q, d, j, p))
                        if a > mid:
                            sum_copy(s, q, d, q, p).wait_recv()
                            value = value + precv[s, d, q, p].astype(F32)
                        elif behind:
                            value = value + weighted(s, q, p, behind)
                    nbr[pl.ds(p * ps, ps), :] = value

    def traces_sent(s):
        for q in range(n):
            for d in range(2):
                for t in range(1, n):
                    if trace_sends(q, d, t) and 0 <= q + 1 - 2 * d < n:
                        for p in range(pieces):
                            later(lambda q=q: c == q, functools.partial(trace_hop, s, q, d, t, p))

    def apply(s, which, k, first):
        owner = owner_at[k]
        if which == "partner":
            shared(s, owner)
            side = 1 - core
        else:
            side = core
        columns = pl.ds(pl.multiple_of(side * rb + owner * shard, 128), shard)
        block = colb[s, side, owner].reshape(shard, ne)
        value = jnp.dot(surf[:, columns], block, preferred_element_type=F32)
        if first:
            acc[...] = value
        else:
            acc[...] += value

    def sum_hop(s, q, d, j, p):
        to = (r, q + 1 if d == 0 else q - 1)
        return remote(sbuf.at[s, d, j, p], rbuf.at[s, d, j, p], r_ss.at[s, d, j, p], r_rs.at[s, d, j, p], to)

    def reduce(s):
        for q in range(n):
            todo = []
            for d in range(2):
                a = q if d == 0 else n - 1 - q
                for b in range(a + 1, n):
                    j = b if d == 0 else n - 1 - b
                    for p in range(2):
                        todo.append((a * 1.8 + (n - 1 - b) * 2 + p, d, j, p))
            todo.sort()

            @pl.when(c == q)
            def _():
                for _, d, j, p in todo:
                    value = part[j, p]
                    if (q if d == 0 else n - 1 - q) > 0:
                        sum_hop(s, q, d, j, p).wait_recv()
                        value = value + rbuf[s, d, j, p].astype(F32)
                    sbuf[s, d, j, p] = value.astype(BF16)
                    sum_hop(s, q, d, j, p).start()
                    later(lambda q=q: c == q, functools.partial(sum_hop, s, q, d, j, p))

    def reduced(s, h):
        for q in range(n):
            @pl.when(c == q)
            def _():
                total = part[q, h]
                for d in range(2):
                    if (q if d == 0 else n - 1 - q) > 0:
                        sum_hop(s, q, d, q, h).wait_recv()
                        total = total + rbuf[s, d, q, h].astype(F32)
                part[q, h] = total
        return part[c, h]

    loads[0].wait()
    if STAGGER:
        @pl.when(core == 1)
        def _():
            for load in loads[1 : 1 + STAGGER]:
                load.wait()
    for h in range(2):
        send_own(0, h, exc[pl.ds(h * hs, hs), :])
    for s in range(ITERS):
        base = exc if s == 0 else sol_ref
        gather(s)

        @pl.when(pos == 0)
        def _():
            colb[s, core] = grp[s]

        if s == 0:
            if STAGGER:
                @pl.when(core == 0)
                def _():
                    for load in loads[1 : 1 + STAGGER]:
                        load.wait()
            else:
                loads[1].wait()
        group = grp[s].reshape(rb, ne)
        for p in range(pieces):
            value = jnp.dot(interp[pl.ds(p * ps, ps), :], group, preferred_element_type=F32)
            trc[s, c, p] = value.astype(BF16)
            send_traces(s, p)
        traces_sent(s)
        chain_relay(s, n)
        if s == 0:
            for load in loads[1 + max(STAGGER, 1) :]:
                load.wait()
        apply(s, "own", 0, True)
        own = trc[s, c].reshape(m, ne)
        combined = jnp.dot(dtn[...], own, preferred_element_type=F32)
        combined = combined + (1.0 + face_weight * NADJ) * own.astype(F32)
        for t in range(1, mid):
            forward_traces(s, t)
        for tick in range(n + 1, 2 * n - 1):
            chain_relay(s, tick)
            apply(s, "own", tick - n, False)
        chain_sent(s)
        trace_sums(s, False)
        for k in range(1 + max(n - 2, 0), n):
            apply(s, "own", k, False)
        for k in range(n):
            apply(s, "partner", k, False)
        trace_sums(s, True)
        turned = (combined - face_weight * nbr[...]).T.astype(BF16)
        volume = jnp.dot(turned, interp[...], preferred_element_type=F32)
        part[...] = (acc[...] + volume.T).reshape(n, 2, hs, ne)
        reduce(s)
        for h in range(2):
            rows = pl.ds(h * hs, hs)
            total = reduced(s, h)
            current = base[rows, :]
            residual = exc[rows, :] - current - total
            updated = current + damping * residual
            if s + 1 < ITERS:
                send_own(s + 1, h, updated)
            res_ref[rows, :] = residual
            sol_ref[rows, :] = updated

    for condition, copy in waits:
        if condition is None:
            copy().wait_send()
        else:
            @pl.when(condition())
            def _():
                copy().wait_send()


def local(surface, excitation, dtn_blocks, interp_blocks, adjacency):
    R, n = lax.axis_size("row"), lax.axis_size("col")
    shard, ne = excitation.shape
    m, rb = interp_blocks.shape[1:]
    hs = shard // 2
    tile = min(512, surface.shape[0])
    pieces = 4
    assert R == 2 * n and n % 2 == 0 and n & (n - 1) == 0
    vmem, hbm = pltpu.VMEM, pl.BlockSpec(memory_space=pl.ANY)
    dma = pltpu.SemaphoreType.DMA
    out = jax.ShapeDtypeStruct((shard, ne), F32)
    S = ITERS
    return pl.pallas_call(
        functools.partial(kernel, R, n, pieces, tile),
        out_shape=(out, out),
        in_specs=[hbm, hbm, hbm, hbm, pl.BlockSpec(memory_space=pltpu.SMEM)],
        out_specs=(pl.BlockSpec(memory_space=vmem),) * 2,
        scratch_shapes=[
            vmem((shard, ne), F32),
            vmem((m, rb), BF16),
            vmem(surface.shape, BF16),
            vmem((m, m), BF16),
            vmem((S, n, 2, hs, ne), BF16),
            vmem((S, 2, n, 2, hs, ne), BF16),
            vmem((S, n, pieces, m // pieces, ne), BF16),
            vmem((rb, ne), F32),
            vmem((n, 2, hs, ne), F32),
            vmem((S, 2, n, 2, hs, ne), BF16),
            vmem((S, 2, n, 2, hs, ne), BF16),
            vmem((m, ne), F32),
            vmem((S, 2, n, pieces, m // pieces, ne), BF16),
            vmem((S, 2, n, pieces, m // pieces, ne), BF16),
            vmem((n, n, 8, ne), F32),
            dma((3 + surface.shape[0] // tile,)),
            *[dma((S, 2, n, 2))] * 2,
            *[dma((S, 2, n, pieces))] * 2,
            *[dma((S, n, 2))] * 4,
            *[dma((S, 2, n, 2))] * 2,
            *[dma((S, 2, n, pieces))] * 2,
            *[dma((n,))] * 2,
        ],
        compiler_params=pltpu.CompilerParams(
            collective_id=0, has_side_effects=True, vmem_limit_bytes=60 * 2**20
        ),
    )(excitation, interp_blocks.reshape(m, rb), surface, dtn_blocks.reshape(m, m), adjacency)


def solution(mesh):
    in_specs = (
        P("row", "col"),
        P(("row", "col"), None),
        P(("row", "col"), None, None),
        P(("row", "col"), None, None),
        P(("row", "col"), None),
    )
    out_specs = (P(("row", "col"), None), P(("row", "col"), None))
    return jax.shard_map(local, mesh=mesh, in_specs=in_specs, out_specs=out_specs, check_vma=False)
```

```python
import functools

import jax
import jax.numpy as jnp
from jax import lax
from jax.experimental import pallas as pl
from jax.experimental.pallas import tpu as pltpu
from jax.sharding import PartitionSpec as P

ITERS = 2
NADJ = 6

damping = 0.25
face_weight = 0.25
F32, BF16 = jnp.float32, jnp.bfloat16


def xor(a, b, bits):
    total = 0
    for i in range(bits):
        x, y = a // 2**i % 2, b // 2**i % 2
        total = total + (x + y - 2 * x * y) * 2**i
    return total


def gray(p, bits):
    return xor(p, p // 2, bits)


def ungray(g, bits):
    total, above = 0, 0
    for i in reversed(range(bits)):
        bit = g // 2**i % 2
        above = above + bit - 2 * above * bit
        total = total + above * 2**i
    return total


def kernel(
    R, n, pieces, tile,
    exc_hbm, interp_hbm, surf_hbm, dtn_hbm, adj,
    cur_ref, tot_ref,
    exc, interp, surf, dtn, grp, colb, trc, acc, part, sbuf, rbuf, ebuf, nbr, psend, precv, cnt,
    load_sem, g_ss, g_rs, t_ss, t_rs, c_ss, c_rs, h_ss, h_rs, r_ss, r_rs, e_rs, p_ss, p_rs, n_ss, n_rs,
):
    bits = n.bit_length() - 1
    mid = n // 2
    _, _, hs, ne = grp.shape[1:]
    m, rb = interp.shape
    shard = 2 * hs
    ps = m // pieces
    r, c = lax.axis_index("row"), lax.axis_index("col")
    core, chip = r % 2, r // 2
    pos = ungray(xor(chip, c, bits), bits)
    partner = (chip * 2 + 1 - core, c)
    gnext = (xor(gray((pos + 1) % n, bits), c, bits) * 2 + core, c)
    gprev = (xor(gray((pos + n - 1) % n, bits), c, bits) * 2 + core, c)

    loads = [
        pltpu.make_async_copy(exc_hbm, exc, load_sem.at[0]),
        pltpu.make_async_copy(interp_hbm, interp, load_sem.at[1]),
    ]
    tiles = surf.shape[0] // tile
    for i in range(tiles):
        rows = pl.ds(i * tile, tile)
        loads.append(pltpu.make_async_copy(surf_hbm.at[rows], surf.at[rows], load_sem.at[3 + i]))
    loads.append(pltpu.make_async_copy(dtn_hbm, dtn, load_sem.at[2]))
    for load in loads:
        load.start()

    def counts_go(q, j):
        return (mid <= q < j) or (j < q <= mid - 1)

    barrier = pltpu.get_barrier_semaphore()
    line = [(r, (c + k) % n) for k in range(1, n)]
    for device in [partner, gnext, gprev] + line:
        pl.semaphore_signal(barrier, inc=1, device_id=device, device_id_type=pl.DeviceIdType.MESH)
    pl.semaphore_wait(barrier, n + 2)

    def remote(src, dst, ss, rs, device):
        return pltpu.make_async_remote_copy(
            src_ref=src, dst_ref=dst, send_sem=ss, recv_sem=rs,
            device_id=device, device_id_type=pl.DeviceIdType.MESH,
        )

    waits = []

    def later(condition, copy):
        waits.append((condition, copy))

    def sender(o, q):
        step = 1 if o < q else -1
        return o if o in (0, n - 1) and (o == 0) == (o < q) or q == o + step else q - step

    def ways(o, q):
        return sorted((k for k in range(n) if k != o and sender(o, k) == q), key=lambda k: -abs(k - o))

    def arrival(o, q):
        if o == q:
            return -1
        a, b = (q, o) if o < q else (n - 1 - q, n - 1 - o)
        return n - a + 1 + 0.3 * a if b == 0 else 2 * (a - b)

    ranks = [sorted(range(n), key=lambda o: arrival(o, q)) for q in range(n)]
    owner_at = []
    for k in range(n):
        owner = ranks[0][k]
        for q in range(1, n):
            owner = jnp.where(c == q, ranks[q][k], owner)
        owner_at.append(owner)

    def block_copy(s, o, q, p):
        block = grp.at[s, o, p]
        return remote(block, block, g_ss.at[s, o, q, p], g_rs.at[s, o, p], (r, q))

    def hops(q, h):
        if (q, h) in ((1, 1), (n - 1, 0)):
            return 1
        return q if h == 0 else n - q

    def passes(q, h, up):
        if q == 0:
            return True
        return up == (h == 0) and (q + 1 <= n - 2 if h == 0 else q - 1 >= 2)

    def chain_copy(src, s, owner, h, up):
        k = 0 if up else 1
        return remote(
            src.at[owner, h], colb.at[s, core, owner, h],
            c_ss.at[s, owner, h, k], c_rs.at[s, owner, h], gnext if up else gprev,
        )

    def share_copy(src, s, owner, h):
        return remote(
            src.at[owner, h], colb.at[s, core, owner, h], h_ss.at[s, owner, h], h_rs.at[s, owner, h], partner
        )

    def chain_source(s, k):
        @pl.when(pos == 0)
        def _():
            for h in range(2):
                for up in (True, False):
                    half = h if up else 1 - h
                    chain_copy(grp.at[s], s, owner_at[k], half, up).start()
            for h in range(2):
                share_copy(grp.at[s], s, owner_at[k], h).start()

    def chain_relay(s, tick):
        for q in range(1, n):
            todo = [(k, h) for k in range(n) for h in range(2) if k + hops(q, h) == tick]
            if not todo:
                continue

            @pl.when(pos == q)
            def _():
                for k, h in todo:
                    src, owner = colb.at[s, core], owner_at[k]
                    chain_copy(src, s, owner, h, True).wait_recv()
                    for up in (True, False):
                        if passes(q, h, up):
                            chain_copy(src, s, owner, h, up).start()
                    share_copy(src, s, owner, h).start()

    def chain_sent(s):
        for owner in range(n):
            for h in range(2):
                later(None, functools.partial(share_copy, colb.at[s, core], s, owner, h))
        for q in range(n):
            for h in range(2):
                for up in (True, False):
                    if passes(q, h, up):
                        for owner in range(n):
                            later(
                                lambda q=q: pos == q,
                                functools.partial(chain_copy, colb.at[s, core], s, owner, h, up),
                            )

    def shared(s, owner):
        for h in range(2):
            block = colb.at[s, 1 - core, owner, h]
            remote(block, block, h_ss.at[s, owner, h], h_rs.at[s, owner, h], partner).wait_recv()

    for p in range(n):
        count = jnp.float32(0)
        for k in range(NADJ):
            count = count + jnp.where(adj[0, k] % n == p, 1.0, 0.0).astype(F32)
        cnt[c, p] = jnp.full((8, ne), count, F32)

    def count_copy(j, q):
        return remote(cnt.at[j], cnt.at[j], n_ss.at[q], n_rs.at[j], (r, q))

    for j in range(n):
        takers = [q for q in range(n) if counts_go(q, j)]
        if takers:
            @pl.when(c == j)
            def _():
                for q in takers:
                    count_copy(j, q).start()
            for q in takers:
                later(lambda j=j: c == j, lambda j=j, q=q: count_copy(j, q))

    def send_own(s, h, value):
        grp[s, c, h] = value.astype(BF16)
        for q in range(n):
            @pl.when(c == q)
            def _():
                for k in ways(q, q):
                    block_copy(s, q, k, h).start()

    def gathered(s):
        for q in range(n):
            for o in range(n):
                for k in ways(o, q):
                    for p in range(2):
                        later(lambda q=q: c == q, functools.partial(block_copy, s, o, k, p))

    def gather(s):
        chain_source(s, 0)
        for rank in range(1, n):
            for q in range(n):
                @pl.when(c == q)
                def _():
                    o = ranks[q][rank]
                    for p in range(2):
                        block_copy(s, o, q, p).wait_recv()
                        for k in ways(o, q):
                            block_copy(s, o, k, p).start()
            chain_source(s, rank)
            chain_relay(s, rank)

    def wanted(o, q):
        return (q if o < q else n - 1 - q) <= mid

    def trace_ways(o, q):
        return [k for k in ways(o, q) if wanted(o, k)]

    def trace_copy(s, o, q, p):
        block = trc.at[s, o, p]
        return remote(block, block, t_ss.at[s, o, q, p], t_rs.at[s, o, p], (r, q))

    def sum_copy(s, q, d, j, p):
        to = (r, q + 1 if d == 0 else q - 1)
        return remote(psend.at[s, d, j, p], precv.at[s, d, j, p], p_ss.at[s, d, j, p], p_rs.at[s, d, j, p], to)

    def send_traces(s, p, far):
        for q in range(n):
            todo = [k for k in trace_ways(q, q) if (abs(k - q) > 1) == far or (far and q not in (0, n - 1))]
            todo = [k for k in todo if far or q in (0, n - 1)]
            if todo:
                @pl.when(c == q)
                def _():
                    for k in todo:
                        trace_copy(s, q, k, p).start()

    def weighted(s, j, p, owners):
        total = None
        for o in owners:
            term = cnt[j, o, 0:1] * trc[s, o, p].astype(F32)
            total = term if total is None else total + term
        return total

    def forward_traces(s):
        for q in range(n):
            todo = [o for o in sorted(range(n), key=lambda o: abs(o - q)) if o != q and trace_ways(o, q)]
            if todo:
                @pl.when(c == q)
                def _():
                    for o in todo:
                        for p in range(pieces):
                            trace_copy(s, o, q, p).wait_recv()
                            for k in trace_ways(o, q):
                                trace_copy(s, o, k, p).start()

    def trace_sums(s, ends):
        for q in range(n):
            far = [d for d in range(2) if (q if d == 0 else n - 1 - q) > mid]
            if bool(far) != ends:
                continue

            @pl.when(c == q)
            def _():
                if s == 0:
                    for j in range(n):
                        if counts_go(q, j):
                            count_copy(j, q).wait_recv()
                for p in range(pieces):
                    value = weighted(s, q, p, [q])
                    for d in range(2):
                        a = q if d == 0 else n - 1 - q
                        behind = list(range(q)) if d == 0 else list(range(q + 1, n))
                        ahead = list(range(n - 1, q, -1)) if d == 0 else list(range(q))
                        if a <= mid:
                            for o in behind:
                                if not trace_ways(o, q):
                                    trace_copy(s, o, q, p).wait_recv()
                        if a >= mid:
                            for j in ahead:
                                if a == mid:
                                    out = weighted(s, j, p, behind + [q])
                                else:
                                    sum_copy(s, q, d, j, p).wait_recv()
                                    out = precv[s, d, j, p].astype(F32) + weighted(s, j, p, [q])
                                psend[s, d, j, p] = out.astype(BF16)
                                sum_copy(s, q, d, j, p).start()
                                later(lambda q=q: c == q, functools.partial(sum_copy, s, q, d, j, p))
                        if a > mid:
                            sum_copy(s, q, d, q, p).wait_recv()
                            value = value + precv[s, d, q, p].astype(F32)
                        elif behind:
                            value = value + weighted(s, q, p, behind)
                    nbr[pl.ds(p * ps, ps), :] = value

    def traces_sent(s):
        for q in range(n):
            for o in range(n):
                for k in trace_ways(o, q):
                    for p in range(pieces):
                        later(lambda q=q: c == q, functools.partial(trace_copy, s, o, k, p))

    def apply(s, which, k, first):
        owner = owner_at[k]
        if which == "partner":
            shared(s, owner)
            side = 1 - core
        else:
            side = core
        columns = pl.ds(pl.multiple_of(side * rb + owner * shard, 128), shard)
        block = colb[s, side, owner].reshape(shard, ne)
        value = jnp.dot(surf[:, columns], block, preferred_element_type=F32)
        if first:
            acc[...] = value
        else:
            acc[...] += value

    def sum_hop(s, q, d, j, p):
        if j in (0, n - 1):
            return remote(sbuf.at[s, d, j, p], ebuf.at[s, q, p], r_ss.at[s, d, j, p], e_rs.at[s, q, p], (r, j))
        to = (r, q + 1 if d == 0 else q - 1)
        return remote(sbuf.at[s, d, j, p], rbuf.at[s, d, j, p], r_ss.at[s, d, j, p], r_rs.at[s, d, j, p], to)

    def reduce(s):
        for q in range(n):
            todo = []
            for d in range(2):
                a = q if d == 0 else n - 1 - q
                for b in range(a + 1, n):
                    j = b if d == 0 else n - 1 - b
                    if b < n - 1:
                        when = n - b + (n if a else 0)
                    else:
                        when = 0 if a else n - 1.5
                    todo += [(when, p, d, j) for p in range(2)]
            todo.sort()

            @pl.when(c == q)
            def _():
                for _, p, d, j in todo:
                    value = part[j, p]
                    if j not in (0, n - 1) and (q if d == 0 else n - 1 - q) > 0:
                        sum_hop(s, q, d, j, p).wait_recv()
                        value = value + rbuf[s, d, j, p].astype(F32)
                    sbuf[s, d, j, p] = value.astype(BF16)
                    sum_hop(s, q, d, j, p).start()
            for _, p, d, j in todo:
                later(lambda q=q: c == q, functools.partial(sum_hop, s, q, d, j, p))

    def reduced(s, h):
        for q in range(n):
            @pl.when(c == q)
            def _():
                total = part[q, h]
                if q in (0, n - 1):
                    for o in sorted(range(n), key=lambda o: abs(o - q))[1:]:
                        sum_hop(s, o, 0 if o < q else 1, q, h).wait_recv()
                        total = total + ebuf[s, o, h].astype(F32)
                else:
                    for d in range(2):
                        sum_hop(s, q, d, q, h).wait_recv()
                        total = total + rbuf[s, d, q, h].astype(F32)
                part[q, h] = total
        return part[c, h]

    loads[0].wait()
    for h in range(2):
        send_own(0, h, exc[pl.ds(h * hs, hs), :])
    for s in range(ITERS):
        gather(s)
        gathered(s)

        @pl.when(pos == 0)
        def _():
            colb[s, core] = grp[s]

        if s == 0:
            loads[1].wait()
        group = grp[s].reshape(rb, ne)
        for p in range(pieces):
            value = jnp.dot(interp[pl.ds(p * ps, ps), :], group, preferred_element_type=F32)
            trc[s, c, p] = value.astype(BF16)
            send_traces(s, p, True)
        for p in range(pieces):
            send_traces(s, p, False)
        traces_sent(s)
        if s == 0:
            for load in loads[2:]:
                load.wait()
        apply(s, "own", 0, True)
        own = trc[s, c].reshape(m, ne)
        combined = jnp.dot(dtn[...], own, preferred_element_type=F32)
        combined = combined + (1.0 + face_weight * NADJ) * own.astype(F32)
        apply(s, "own", 1, False)
        chain_relay(s, n)
        forward_traces(s)
        trace_sums(s, False)
        for tick in range(n + 1, 2 * n - 2):
            chain_relay(s, tick)
        chain_sent(s)
        for k in range(2, n):
            apply(s, "own", k, False)
        for k in range(n):
            apply(s, "partner", k, False)
        trace_sums(s, True)
        turned = (combined - face_weight * nbr[...]).T.astype(BF16)
        volume = jnp.dot(turned, interp[...], preferred_element_type=F32)
        part[...] = (acc[...] + volume.T).reshape(n, 2, hs, ne)
        reduce(s)
        for h in range(2):
            rows = pl.ds(h * hs, hs)
            total = reduced(s, h)
            if s + 1 < ITERS:
                current = exc[rows, :] if s == 0 else cur_ref[rows, :]
                updated = current + damping * (exc[rows, :] - current - total)
                send_own(s + 1, h, updated)
                cur_ref[rows, :] = updated
            else:
                tot_ref[rows, :] = total

    for condition, copy in waits:
        if condition is None:
            copy().wait_send()
        else:
            @pl.when(condition())
            def _():
                copy().wait_send()


def local(surface, excitation, dtn_blocks, interp_blocks, adjacency):
    R, n = lax.axis_size("row"), lax.axis_size("col")
    shard, ne = excitation.shape
    m, rb = interp_blocks.shape[1:]
    hs = shard // 2
    tile = min(512, surface.shape[0])
    pieces = 4
    assert R == 2 * n and n >= 4 and n & (n - 1) == 0
    vmem, hbm = pltpu.VMEM, pl.BlockSpec(memory_space=pl.ANY)
    dma = pltpu.SemaphoreType.DMA
    out = jax.ShapeDtypeStruct((shard, ne), F32)
    S = ITERS
    current, total = pl.pallas_call(
        functools.partial(kernel, R, n, pieces, tile),
        out_shape=(out, out),
        in_specs=[hbm, hbm, hbm, hbm, pl.BlockSpec(memory_space=pltpu.SMEM)],
        out_specs=(pl.BlockSpec(memory_space=vmem),) * 2,
        scratch_shapes=[
            vmem((shard, ne), F32),
            vmem((m, rb), BF16),
            vmem(surface.shape, BF16),
            vmem((m, m), BF16),
            vmem((S, n, 2, hs, ne), BF16),
            vmem((S, 2, n, 2, hs, ne), BF16),
            vmem((S, n, pieces, m // pieces, ne), BF16),
            vmem((rb, ne), F32),
            vmem((n, 2, hs, ne), F32),
            vmem((S, 2, n, 2, hs, ne), BF16),
            vmem((S, 2, n, 2, hs, ne), BF16),
            vmem((S, n, 2, hs, ne), BF16),
            vmem((m, ne), F32),
            vmem((S, 2, n, pieces, m // pieces, ne), BF16),
            vmem((S, 2, n, pieces, m // pieces, ne), BF16),
            vmem((n, n, 8, ne), F32),
            dma((3 + surface.shape[0] // tile,)),
            dma((S, n, n, 2)),
            dma((S, n, 2)),
            dma((S, n, n, pieces)),
            dma((S, n, pieces)),
            dma((S, n, 2, 2)),
            *[dma((S, n, 2))] * 3,
            *[dma((S, 2, n, 2))] * 2,
            dma((S, n, 2)),
            *[dma((S, 2, n, pieces))] * 2,
            *[dma((n,))] * 2,
        ],
        compiler_params=pltpu.CompilerParams(
            collective_id=0, has_side_effects=True, vmem_limit_bytes=60 * 2**20
        ),
    )(excitation, interp_blocks.reshape(m, rb), surface, dtn_blocks.reshape(m, m), adjacency)
    residual = excitation - current - total
    return current + damping * residual, residual


def solution(mesh):
    in_specs = (
        P("row", "col"),
        P(("row", "col"), None),
        P(("row", "col"), None, None),
        P(("row", "col"), None, None),
        P(("row", "col"), None),
    )
    out_specs = (P(("row", "col"), None), P(("row", "col"), None))
    return jax.shard_map(local, mesh=mesh, in_specs=in_specs, out_specs=out_specs, check_vma=False)
```

```python
import functools

import jax
import jax.numpy as jnp
from jax import lax
from jax.experimental import pallas as pl
from jax.experimental.pallas import tpu as pltpu
from jax.sharding import PartitionSpec as P

ITERS = 2
NADJ = 6

damping = 0.25
face_weight = 0.25
F32, BF16 = jnp.float32, jnp.bfloat16


def xor(a, b, bits):
    total = 0
    for i in range(bits):
        x, y = a // 2**i % 2, b // 2**i % 2
        total = total + (x + y - 2 * x * y) * 2**i
    return total


def gray(p, bits):
    return xor(p, p // 2, bits)


def ungray(g, bits):
    total, above = 0, 0
    for i in reversed(range(bits)):
        bit = g // 2**i % 2
        above = above + bit - 2 * above * bit
        total = total + above * 2**i
    return total


def kernel(
    R, n, pieces, tile,
    exc_hbm, interp_hbm, surf_hbm, dtn_hbm, adj,
    cur_ref, tot_ref,
    exc, interp, surf, dtn, grp, colb, trc, acc, part, sbuf, rbuf, ebuf, nbr, psend, precv, cnt,
    load_sem, g_ss, g_rs, t_ss, t_rs, c_ss, c_rs, h_ss, h_rs, r_ss, r_rs, e_rs, p_ss, p_rs, n_ss, n_rs,
):
    bits = n.bit_length() - 1
    mid = n // 2
    _, _, hs, ne = grp.shape[1:]
    m, rb = interp.shape
    shard = 2 * hs
    ps = m // pieces
    r, c = lax.axis_index("row"), lax.axis_index("col")
    core, chip = r % 2, r // 2
    pos = ungray(xor(chip, c, bits), bits)
    partner = (chip * 2 + 1 - core, c)
    gnext = (xor(gray((pos + 1) % n, bits), c, bits) * 2 + core, c)
    gprev = (xor(gray((pos + n - 1) % n, bits), c, bits) * 2 + core, c)

    loads = [
        pltpu.make_async_copy(exc_hbm, exc, load_sem.at[0]),
        pltpu.make_async_copy(interp_hbm, interp, load_sem.at[1]),
    ]
    tiles = surf.shape[0] // tile
    for i in range(tiles):
        rows = pl.ds(i * tile, tile)
        loads.append(pltpu.make_async_copy(surf_hbm.at[rows], surf.at[rows], load_sem.at[3 + i]))
    loads.append(pltpu.make_async_copy(dtn_hbm, dtn, load_sem.at[2]))
    loads[0].start()

    def counts_go(q, j):
        return (mid <= q < j) or (j < q <= mid - 1)

    barrier = pltpu.get_barrier_semaphore()
    line = [(r, (c + k) % n) for k in range(1, n)]
    for device in [partner, gnext, gprev] + line:
        pl.semaphore_signal(barrier, inc=1, device_id=device, device_id_type=pl.DeviceIdType.MESH)
    pl.semaphore_wait(barrier, n + 2)

    def remote(src, dst, ss, rs, device):
        return pltpu.make_async_remote_copy(
            src_ref=src, dst_ref=dst, send_sem=ss, recv_sem=rs,
            device_id=device, device_id_type=pl.DeviceIdType.MESH,
        )

    waits = {None: []}

    def later(condition, copy):
        waits.setdefault(condition, []).append(copy)

    def sender(o, q):
        step = 1 if o < q else -1
        return o if o in (0, n - 1) and (o == 0) == (o < q) or q == o + step else q - step

    def ways(o, q):
        return [k for k in (q - 1, q + 1) if 0 <= k < n and abs(k - o) > abs(q - o)]

    def arrival(o, q):
        if o == q:
            return -1
        return abs(o - q)

    ranks = [sorted(range(n), key=lambda o: arrival(o, q)) for q in range(n)]
    owner_at = []
    for k in range(n):
        owner = ranks[0][k]
        for q in range(1, n):
            owner = jnp.where(c == q, ranks[q][k], owner)
        owner_at.append(owner)

    def block_copy(s, o, q, p):
        block = grp.at[s, o, p]
        return remote(block, block, g_ss.at[s, o, q, p], g_rs.at[s, o, p], (r, q))

    def hops(q, h):
        if (q, h) in ((1, 1), (n - 1, 0)):
            return 1
        return q if h == 0 else n - q

    def passes(q, h, up):
        if q == 0:
            return True
        return up == (h == 0) and (q + 1 <= n - 2 if h == 0 else q - 1 >= 2)

    def chain_copy(src, s, owner, h, up):
        k = 0 if up else 1
        return remote(
            src.at[owner, h], colb.at[s, core, owner, h],
            c_ss.at[s, owner, h, k], c_rs.at[s, owner, h], gnext if up else gprev,
        )

    def share_copy(src, s, owner, h):
        return remote(
            src.at[owner, h], colb.at[s, core, owner, h], h_ss.at[s, owner, h], h_rs.at[s, owner, h], partner
        )

    def chain_source(s, k):
        @pl.when(pos == 0)
        def _():
            for h in range(2):
                for up in (True, False):
                    half = h if up else 1 - h
                    chain_copy(grp.at[s], s, owner_at[k], half, up).start()
            for h in range(2):
                share_copy(grp.at[s], s, owner_at[k], h).start()

    def chain_relay(s, tick):
        for q in range(1, n):
            todo = [(k, h) for k in range(n) for h in range(2) if k + hops(q, h) == tick]
            if not todo:
                continue

            @pl.when(pos == q)
            def _():
                for k, h in todo:
                    src, owner = colb.at[s, core], owner_at[k]
                    chain_copy(src, s, owner, h, True).wait_recv()
                    for up in (True, False):
                        if passes(q, h, up):
                            chain_copy(src, s, owner, h, up).start()
                    share_copy(src, s, owner, h).start()

    def chain_sent(s):
        for owner in range(n):
            for h in range(2):
                later(None, functools.partial(share_copy, colb.at[s, core], s, owner, h))
        for q in range(n):
            for h in range(2):
                for up in (True, False):
                    if passes(q, h, up):
                        for owner in range(n):
                            later(
                                ("pos", q),
                                functools.partial(chain_copy, colb.at[s, core], s, owner, h, up),
                            )

    def shared(s, owner):
        for h in range(2):
            block = colb.at[s, 1 - core, owner, h]
            remote(block, block, h_ss.at[s, owner, h], h_rs.at[s, owner, h], partner).wait_recv()

    for p in range(n):
        count = jnp.float32(0)
        for k in range(NADJ):
            count = count + jnp.where(adj[0, k] % n == p, 1.0, 0.0).astype(F32)
        cnt[c, p] = jnp.full((8, ne), count, F32)

    def count_copy(j, q):
        return remote(cnt.at[j], cnt.at[j], n_ss.at[q], n_rs.at[j], (r, q))

    for j in range(n):
        takers = [q for q in range(n) if counts_go(q, j)]
        if takers:
            @pl.when(c == j)
            def _():
                for q in takers:
                    count_copy(j, q).start()
            for q in takers:
                later(("c", j), lambda j=j, q=q: count_copy(j, q))

    def send_own(s, h, value):
        grp[s, c, h] = value.astype(BF16)
        for q in range(n):
            @pl.when(c == q)
            def _():
                for k in ways(q, q):
                    block_copy(s, q, k, h).start()

    def gathered(s):
        for q in range(n):
            for o in range(n):
                for k in ways(o, q):
                    for p in range(2):
                        later(("c", q), functools.partial(block_copy, s, o, k, p))

    def gather(s):
        chain_source(s, 0)
        for rank in range(1, n):
            for q in range(n):
                @pl.when(c == q)
                def _():
                    o = ranks[q][rank]
                    for p in range(2):
                        block_copy(s, o, q, p).wait_recv()
                        for k in ways(o, q):
                            block_copy(s, o, k, p).start()
            chain_source(s, rank)
            chain_relay(s, rank)

    def wanted(o, q):
        return (q if o < q else n - 1 - q) <= mid

    def trace_ways(o, q):
        near = [k for k in range(n) if k != o and sender(o, k) == q]
        return [k for k in sorted(near, key=lambda k: -abs(k - o)) if wanted(o, k)]

    def trace_copy(s, o, q, p):
        block = trc.at[s, o, p]
        return remote(block, block, t_ss.at[s, o, q, p], t_rs.at[s, o, p], (r, q))

    def sum_copy(s, q, d, j, p):
        to = (r, q + 1 if d == 0 else q - 1)
        return remote(psend.at[s, d, j, p], precv.at[s, d, j, p], p_ss.at[s, d, j, p], p_rs.at[s, d, j, p], to)

    def send_traces(s, p, far):
        for q in range(n):
            todo = [k for k in trace_ways(q, q) if (abs(k - q) > 1) == far or (far and q not in (0, n - 1))]
            todo = [k for k in todo if far or q in (0, n - 1)]
            if todo:
                @pl.when(c == q)
                def _():
                    for k in todo:
                        trace_copy(s, q, k, p).start()

    def weighted(s, j, p, owners):
        total = None
        for o in owners:
            term = cnt[j, o, 0:1] * trc[s, o, p].astype(F32)
            total = term if total is None else total + term
        return total

    def forward_traces(s):
        for q in range(n):
            todo = [o for o in sorted(range(n), key=lambda o: abs(o - q)) if o != q and trace_ways(o, q)]
            if todo:
                @pl.when(c == q)
                def _():
                    for o in todo:
                        for p in range(pieces):
                            trace_copy(s, o, q, p).wait_recv()
                            for k in trace_ways(o, q):
                                trace_copy(s, o, k, p).start()

    def trace_sums(s, ends):
        for q in range(n):
            far = [d for d in range(2) if (q if d == 0 else n - 1 - q) > mid]
            if bool(far) != ends:
                continue

            @pl.when(c == q)
            def _():
                if s == 0:
                    for j in range(n):
                        if counts_go(q, j):
                            count_copy(j, q).wait_recv()
                for p in range(pieces):
                    value = weighted(s, q, p, [q])
                    for d in range(2):
                        a = q if d == 0 else n - 1 - q
                        behind = list(range(q)) if d == 0 else list(range(q + 1, n))
                        ahead = list(range(n - 1, q, -1)) if d == 0 else list(range(q))
                        if a <= mid:
                            for o in behind:
                                if not trace_ways(o, q):
                                    trace_copy(s, o, q, p).wait_recv()
                        if a >= mid:
                            for j in ahead:
                                if a == mid:
                                    out = weighted(s, j, p, behind + [q])
                                else:
                                    sum_copy(s, q, d, j, p).wait_recv()
                                    out = precv[s, d, j, p].astype(F32) + weighted(s, j, p, [q])
                                psend[s, d, j, p] = out.astype(BF16)
                                sum_copy(s, q, d, j, p).start()
                                later(("c", q), functools.partial(sum_copy, s, q, d, j, p))
                        if a > mid:
                            sum_copy(s, q, d, q, p).wait_recv()
                            value = value + precv[s, d, q, p].astype(F32)
                        elif behind:
                            value = value + weighted(s, q, p, behind)
                    nbr[pl.ds(p * ps, ps), :] = value

    def traces_sent(s):
        for q in range(n):
            for o in range(n):
                for k in trace_ways(o, q):
                    for p in range(pieces):
                        later(("c", q), functools.partial(trace_copy, s, o, k, p))

    def apply(s, which, k, first):
        owner = owner_at[k]
        if which == "partner":
            shared(s, owner)
            side = 1 - core
        else:
            side = core
        columns = pl.ds(pl.multiple_of(side * rb + owner * shard, 128), shard)
        block = colb[s, side, owner].reshape(shard, ne)
        value = jnp.dot(surf[:, columns], block, preferred_element_type=F32)
        if first:
            acc[...] = value
        else:
            acc[...] += value

    def sum_hop(s, q, d, j, p):
        if j in (0, n - 1):
            return remote(sbuf.at[s, d, j, p], ebuf.at[s, q, p], r_ss.at[s, d, j, p], e_rs.at[s, q, p], (r, j))
        to = (r, q + 1 if d == 0 else q - 1)
        return remote(sbuf.at[s, d, j, p], rbuf.at[s, d, j, p], r_ss.at[s, d, j, p], r_rs.at[s, d, j, p], to)

    def reduce(s):
        for q in range(n):
            todo = []
            for d in range(2):
                a = q if d == 0 else n - 1 - q
                for b in range(a + 1, n):
                    j = b if d == 0 else n - 1 - b
                    if b < n - 1:
                        when = n - b + (n if a else 0)
                    else:
                        when = 0 if a else n - 1.5
                    todo += [(when, p, d, j) for p in range(2)]
            todo.sort()

            @pl.when(c == q)
            def _():
                for _, p, d, j in todo:
                    value = part[j, p]
                    if j not in (0, n - 1) and (q if d == 0 else n - 1 - q) > 0:
                        sum_hop(s, q, d, j, p).wait_recv()
                        value = value + rbuf[s, d, j, p].astype(F32)
                    sbuf[s, d, j, p] = value.astype(BF16)
                    sum_hop(s, q, d, j, p).start()
            for _, p, d, j in todo:
                later(("c", q), functools.partial(sum_hop, s, q, d, j, p))

    def reduced(s, h):
        for q in range(n):
            @pl.when(c == q)
            def _():
                total = part[q, h]
                if q in (0, n - 1):
                    for o in sorted(range(n), key=lambda o: abs(o - q))[1:]:
                        sum_hop(s, o, 0 if o < q else 1, q, h).wait_recv()
                        total = total + ebuf[s, o, h].astype(F32)
                else:
                    for d in range(2):
                        sum_hop(s, q, d, q, h).wait_recv()
                        total = total + rbuf[s, d, q, h].astype(F32)
                part[q, h] = total
        return part[c, h]

    loads[0].wait()
    for load in loads[1:]:
        load.start()
    for h in range(2):
        send_own(0, h, exc[pl.ds(h * hs, hs), :])
    for s in range(ITERS):
        gather(s)
        gathered(s)

        @pl.when(pos == 0)
        def _():
            colb[s, core] = grp[s]

        if s == 0:
            loads[1].wait()
        group = grp[s].reshape(rb, ne)
        for p in range(pieces):
            value = jnp.dot(interp[pl.ds(p * ps, ps), :], group, preferred_element_type=F32)
            trc[s, c, p] = value.astype(BF16)
            send_traces(s, p, True)
        for p in range(pieces):
            send_traces(s, p, False)
        traces_sent(s)
        if s == 0:
            for load in loads[2:]:
                load.wait()
        apply(s, "own", 0, True)
        own = trc[s, c].reshape(m, ne)
        combined = jnp.dot(dtn[...], own, preferred_element_type=F32)
        combined = combined + (1.0 + face_weight * NADJ) * own.astype(F32)
        apply(s, "own", 1, False)
        chain_relay(s, n)
        forward_traces(s)
        trace_sums(s, False)
        for tick in range(n + 1, 2 * n - 2):
            chain_relay(s, tick)
        chain_sent(s)
        for k in range(2, n):
            apply(s, "own", k, False)
        for k in range(n):
            apply(s, "partner", k, False)
        trace_sums(s, True)
        turned = (combined - face_weight * nbr[...]).T.astype(BF16)
        volume = jnp.dot(turned, interp[...], preferred_element_type=F32)
        part[...] = (acc[...] + volume.T).reshape(n, 2, hs, ne)
        reduce(s)
        for h in range(2):
            rows = pl.ds(h * hs, hs)
            total = reduced(s, h)
            if s + 1 < ITERS:
                current = exc[rows, :] if s == 0 else cur_ref[rows, :]
                updated = current + damping * (exc[rows, :] - current - total)
                send_own(s + 1, h, updated)
                cur_ref[rows, :] = updated
            else:
                tot_ref[rows, :] = total

    for copy in waits.pop(None):
        copy().wait_send()
    for (axis, q), copies in waits.items():
        @pl.when((c if axis == "c" else pos) == q)
        def _():
            for copy in copies:
                copy().wait_send()


def local(surface, excitation, dtn_blocks, interp_blocks, adjacency):
    R, n = lax.axis_size("row"), lax.axis_size("col")
    shard, ne = excitation.shape
    m, rb = interp_blocks.shape[1:]
    hs = shard // 2
    tile = min(512, surface.shape[0])
    pieces = 4
    assert R == 2 * n and n >= 4 and n & (n - 1) == 0
    vmem, hbm = pltpu.VMEM, pl.BlockSpec(memory_space=pl.ANY)
    dma = pltpu.SemaphoreType.DMA
    out = jax.ShapeDtypeStruct((shard, ne), F32)
    S = ITERS
    current, total = pl.pallas_call(
        functools.partial(kernel, R, n, pieces, tile),
        out_shape=(out, out),
        in_specs=[hbm, hbm, hbm, hbm, pl.BlockSpec(memory_space=pltpu.SMEM)],
        out_specs=(pl.BlockSpec(memory_space=vmem),) * 2,
        scratch_shapes=[
            vmem((shard, ne), F32),
            vmem((m, rb), BF16),
            vmem(surface.shape, BF16),
            vmem((m, m), BF16),
            vmem((S, n, 2, hs, ne), BF16),
            vmem((S, 2, n, 2, hs, ne), BF16),
            vmem((S, n, pieces, m // pieces, ne), BF16),
            vmem((rb, ne), F32),
            vmem((n, 2, hs, ne), F32),
            vmem((S, 2, n, 2, hs, ne), BF16),
            vmem((S, 2, n, 2, hs, ne), BF16),
            vmem((S, n, 2, hs, ne), BF16),
            vmem((m, ne), F32),
            vmem((S, 2, n, pieces, m // pieces, ne), BF16),
            vmem((S, 2, n, pieces, m // pieces, ne), BF16),
            vmem((n, n, 8, ne), F32),
            dma((3 + surface.shape[0] // tile,)),
            dma((S, n, n, 2)),
            dma((S, n, 2)),
            dma((S, n, n, pieces)),
            dma((S, n, pieces)),
            dma((S, n, 2, 2)),
            *[dma((S, n, 2))] * 3,
            *[dma((S, 2, n, 2))] * 2,
            dma((S, n, 2)),
            *[dma((S, 2, n, pieces))] * 2,
            *[dma((n,))] * 2,
        ],
        compiler_params=pltpu.CompilerParams(
            collective_id=0, has_side_effects=True, vmem_limit_bytes=60 * 2**20
        ),
    )(excitation, interp_blocks.reshape(m, rb), surface, dtn_blocks.reshape(m, m), adjacency)
    residual = excitation - current - total
    return current + damping * residual, residual


def solution(mesh):
    in_specs = (
        P("row", "col"),
        P(("row", "col"), None),
        P(("row", "col"), None, None),
        P(("row", "col"), None, None),
        P(("row", "col"), None),
    )
    out_specs = (P(("row", "col"), None), P(("row", "col"), None))
    return jax.shard_map(local, mesh=mesh, in_specs=in_specs, out_specs=out_specs, check_vma=False)
```
